32 devices in a mesh: scen: 8 (over z, y), gen: 4 (over x, core).
Axes of the slice: x: 2, y: 2, z: 4, core: 2. Of those that a mesh axis runs over, the one named last changes fastest.
Arguments:
- zone_load: float32 [128, 16, 256], P('scen'), may hold values from 0.3 to 1
- linear_cost: float32 [16, 20480], P(None, 'gen'), may hold values from -4 to 4
- cost_diag: float32 [20480], P('gen'), may hold values from 0.5 to 2
- capacity: float32 [20480], P('gen'), may hold values from 0.5 to 2
- cost_tiles: bfloat16 [80, 256, 256], P('gen'), may hold values from -0.375 to 0.375
- coupling_tiles: bfloat16 [8, 80, 256, 256], P('scen', 'gen'), may hold values from -0.375 to 0.375
- block_map: int32 [8, 80], P('scen', 'gen'), may hold values 0 or 1
- zone_index: int32 [20480], P('gen'), may hold values from 0 to 255
- step_numer: int32 [5], replicated, may hold values from 1 to 4
- step_denom: int32 [5], replicated, may hold values from 5 to 8
Outputs:
- dispatch: float32 [128, 16, 20480], P('scen', None, 'gen')
- prices: float32 [128, 16, 256], P('scen')
- plan: float32 [16, 20480], P(None, 'gen')
The draws below stay inside these ranges and needn't reach their ends.
All inputs are finite; a program needn't handle non-finite values. No bound on the sum of `block_map` on one device may be relied on, other than what follows from the above.
Results may differ from the reference program's by a relative error of at most 0.0003.
Values sent between devices are 32-bit elements; how exact they have to be, the bound alone decides.
No kernel may reach another device: no remote copies, remote signals or barrier semaphores. Data moves between devices by JAX's collectives and lax.ppermute only.
A program may use at most 128 MiB of HBM per device.

```python
import math
import jax
import jax.numpy as jnp
from jax import lax

S_DEV = 16
P_SIZE = 16
G = 20480
TILE = 256
ZONES = 256
ITERS = 5
S = 128
GB = 80
SBLOCKS = 8


def plant(result, key, low, top_value):
    dims = result.shape
    place = [jax.random.randint(jax.random.fold_in(key, axis), (), 0, dims[axis]) for axis in range(len(dims))]
    result = result.at[tuple(place)].set(low)
    longest = dims.index(max(dims))
    place[longest] = (place[longest] + 1) % dims[longest]
    return result.at[tuple(place)].set(top_value)


def level_of(rng, shape, pieces, smallest, largest):
    level = 1.0
    for position, shards_of in pieces:
        draws = jax.random.uniform(jax.random.fold_in(jax.random.fold_in(rng, 6), position), (shards_of,), jnp.float32, smallest / len(pieces), largest / len(pieces))
        level = level * jnp.repeat(jnp.exp(draws), shape[position] // shards_of).reshape((-1,) + (1,) * (len(shape) - 1 - position))
    return level


def bell_draw(stream_key, extent, scale, bound, shards=(), kind=jnp.bfloat16):
    values = scale * jax.random.normal(stream_key, extent, jnp.float32)
    if shards:
        values = values * level_of(stream_key, extent, shards, -0.22, 0.18)
    return jnp.clip(values, -bound, bound).astype(kind)


def setup_inputs(seed: int = 0) -> dict:
    seeds = jax.random.split(jax.random.key(seed), 11)
    zone_load = jnp.clip(0.3 + 0.7 * jax.random.uniform(seeds[0], (S, P_SIZE, ZONES), jnp.float32) ** level_of(seeds[0], (S, P_SIZE, ZONES), ((0, 8),), -0.2, 0.2), 0.3, 1.0)
    linear_cost = bell_draw(seeds[1], (P_SIZE, G), 1.0, 4.0, ((1, 4),), jnp.float32)
    cost_diag = jnp.clip(jnp.exp(math.log(2.0) - 1.3862944 * jax.random.uniform(seeds[2], (G,), jnp.float32) ** level_of(seeds[2], (G,), ((0, 4),), -0.2, 0.2)), 0.5, 2.0)
    capacity = jnp.clip(jnp.exp(math.log(2.0) - 1.3862944 * jax.random.uniform(seeds[3], (G,), jnp.float32) ** level_of(seeds[3], (G,), ((0, 4),), -0.2, 0.2)), 0.5, 2.0)
    cost_tiles = bell_draw(seeds[4], (GB, TILE, TILE), TILE ** -0.5, 0.375, ((0, 4),))
    coupling_tiles = bell_draw(seeds[5], (SBLOCKS, GB, TILE, TILE), TILE ** -0.5, 0.375, ((0, 8), (1, 4)))
    block_map = plant((jax.random.randint(seeds[6], (SBLOCKS, GB), 0, 2) < 1).astype(jnp.int32), jax.random.fold_in(seeds[6], 1), 0, 1)
    zone_index = plant(jax.random.randint(seeds[7], (G,), 0, ZONES), jax.random.fold_in(seeds[7], 1), 0, ZONES - 1).astype(jnp.int32)
    step_numer = plant(jax.random.randint(seeds[8], (ITERS,), 1, 5), jax.random.fold_in(seeds[8], 1), 1, 4).astype(jnp.int32)
    step_denom = plant(jax.random.randint(seeds[9], (ITERS,), 5, 9), jax.random.fold_in(seeds[9], 1), 5, 8).astype(jnp.int32)
    return dict(zone_load=zone_load, linear_cost=linear_cost, cost_diag=cost_diag, capacity=capacity, cost_tiles=cost_tiles, coupling_tiles=coupling_tiles, block_map=block_map, zone_index=zone_index, step_numer=step_numer, step_denom=step_denom)


penalty = 2.0
centering = 0.5
epsilon = 1e-06

def tile_products(dispatch_block, cost_tiles, coupling, block_mask):
    rounded = lax.optimization_barrier(dispatch_block.astype(jnp.bfloat16))
    row_data = rounded.reshape(S_DEV * P_SIZE, GB, TILE).astype(jnp.float32)
    own_part = jnp.einsum('rki,kij->rkj', row_data, cost_tiles.astype(jnp.float32))
    cross_part = jnp.einsum('rki,kij->rkj', row_data, coupling.astype(jnp.float32))
    combined = own_part + cross_part * block_mask.astype(jnp.float32)[None, :, None]
    return combined.reshape(S_DEV, P_SIZE, G)

def reference(zone_load, linear_cost, cost_diag, capacity, cost_tiles, coupling_tiles, block_map, zone_index, step_numer, step_denom):
    blocks = S // S_DEV
    levels = 0.2 + 0.6 * (jnp.arange(S, dtype=jnp.float32) + 0.5) / S
    dispatch = (levels.reshape(blocks, S_DEV, 1, 1) * capacity).astype(jnp.float32)
    dispatch = jnp.broadcast_to(dispatch, (blocks, S_DEV, P_SIZE, G))
    low_dual = jnp.ones((blocks, S_DEV, P_SIZE, G), jnp.float32)
    high_dual = jnp.ones((blocks, S_DEV, P_SIZE, G), jnp.float32)
    prices = jnp.zeros((S, P_SIZE, ZONES), jnp.float32)
    lowest = 0.02 * capacity
    highest = 0.98 * capacity
    plan = jnp.zeros((P_SIZE, G), jnp.float32)
    for iteration in range(ITERS):
        step_size = step_numer[iteration].astype(jnp.float32) / step_denom[iteration].astype(jnp.float32)
        plan = lax.optimization_barrier(jnp.sum(dispatch, axis=(0, 1))) / S
        flattened = dispatch.reshape(S * P_SIZE, G)
        totals = jnp.zeros((S * P_SIZE, ZONES), jnp.float32).at[:, zone_index].add(flattened)
        imbalance = totals.reshape(S, P_SIZE, ZONES) * (ZONES / G) - zone_load
        price_blocks = prices.reshape(blocks, S_DEV, P_SIZE, ZONES)

        def residual_block(inputs):
            dispatch_block, low_block, high_block, price_block, coupling, block_mask = inputs
            products = tile_products(dispatch_block, cost_tiles, coupling, block_mask)
            return cost_diag * dispatch_block + products + linear_cost + penalty * (dispatch_block - plan) + price_block[..., zone_index] - low_block + high_block
        residual = lax.map(residual_block, (dispatch, low_dual, high_dual, price_blocks, coupling_tiles, block_map))
        gap_sum = jnp.sum(dispatch * low_dual + (capacity - dispatch) * high_dual)
        dual_sq = jnp.sum(residual * residual)
        primal_sq = jnp.sum(imbalance * imbalance)
        target = centering * gap_sum / (2.0 * S * P_SIZE * G)
        dual_rms = jnp.sqrt(dual_sq / (S * P_SIZE * G) + epsilon)
        primal_rms = jnp.sqrt(primal_sq / (S * P_SIZE * ZONES) + epsilon)
        scaling = cost_diag + penalty + low_dual / dispatch + high_dual / (capacity - dispatch)
        updated = jnp.clip(dispatch - step_size * residual / (scaling * (1.0 + dual_rms)), lowest, highest)
        low_dual = low_dual + step_size * (target / updated - low_dual)
        high_dual = high_dual + step_size * (target / (capacity - updated) - high_dual)
        prices = prices + step_size * imbalance / (1.0 + primal_rms)
        dispatch = updated
    return (dispatch.reshape(S, P_SIZE, G), prices, plan)
```

```python
import functools

import jax
import jax.numpy as jnp
import numpy as np
from jax import lax
from jax.experimental import pallas as pl
from jax.experimental.pallas import tpu as pltpu
from jax.sharding import PartitionSpec as P

PENALTY = 2.0
CENTERING = 0.5
EPSILON = 1e-06
LANES = 128

F32 = jnp.float32
BF16 = jnp.bfloat16
NT = (((1,), (1,)), ((), ()))
NN = (((1,), (0,)), ((), ()))


def dot(a, b, dims):
    return lax.dot_general(a, b, dims, preferred_element_type=F32)


def split(x):
    hi = x.astype(BF16)
    return hi, (x - hi.astype(F32)).astype(BF16)


def lane(row, i):
    return row[:, i : i + 1]


def zone_rows(zone_ref, cols, size, zones):
    ids = lax.broadcasted_iota(jnp.int32, (zones, size), 0)
    return (ids == zone_ref[:, cols]).astype(BF16)


def total(x):
    return jnp.sum(jnp.sum(x, axis=1, keepdims=True), axis=0, keepdims=True)


def stage(body, n_small, n_large, n_small_out, n_large_out, extra):
    def kernel(*refs):
        refs = list(refs)

        def take(n):
            out = refs[:n]
            del refs[:n]
            return out

        first, small, large = take(extra), take(n_small), take(n_large)
        small_out, large_out = take(n_small_out), take(n_large_out)
        held, made = take(n_small), take(n_small_out)
        in_sems, out_sems = take(2)
        loads = [pltpu.make_async_copy(a, b, in_sems.at[j]) for j, (a, b) in enumerate(zip(small, held))]
        for copy in loads:
            copy.start()

        def ready():
            for copy in loads:
                copy.wait()

        finish = body(ready, first, held, large, made, large_out, refs)
        stores = [pltpu.make_async_copy(b, a, out_sems.at[j]) for j, (a, b) in enumerate(zip(small_out, made))]
        for copy in stores:
            copy.start()
        finish()
        for copy in stores:
            copy.wait()

    return kernel


def staged_call(
    body, first, small, large, small_out, large_out, scratch, name, cost=None, aliases=None
):
    dma = pltpu.SemaphoreType.DMA
    hbm = pl.BlockSpec(memory_space=pl.ANY)
    begin = len(first) + len(small)
    alias = {begin + a: len(small_out) + b for a, b in (aliases or {}).items()}
    return pl.pallas_call(
        stage(body, len(small), len(large), len(small_out), len(large_out), len(first)),
        in_specs=[pl.BlockSpec(memory_space=pltpu.SMEM)] * len(first) + [hbm] * (len(small) + len(large)),
        out_specs=[hbm] * (len(small_out) + len(large_out)),
        out_shape=small_out + large_out,
        scratch_shapes=[pltpu.VMEM(v.shape, v.dtype) for v in small + small_out]
        + [dma((max(1, len(small)),)), dma((max(1, len(small_out)),))]
        + scratch,
        input_output_aliases=alias,
        compiler_params=params(60),
        cost_estimate=cost,
        name=name,
    )(*first, *small, *large)


def lanes(c, width, t=0, size=None):
    return pl.ds(pl.multiple_of(c * width + t, LANES), width if size is None else size)


def first_body(dims, ready, first, small, large, made, large_out, scratch):
    (mask_ref,) = first
    level_ref, load_ref, lin_ref, diag_ref, cap_ref, zone_ref = small
    cost_in, coup_in = large
    base_ref, pack_ref = made
    sums, capz, cost, coup, sems = scratch
    ns, periods = dims.local_scen, dims.periods
    zones = load_ref.shape[1]
    chunks, per, tile = cost.shape[:3]

    def copies(c):
        return [
            pltpu.make_async_copy(source.at[c], target.at[c], sems.at[j, c])
            for j, (source, target) in enumerate([(cost_in, cost), (coup_in, coup)])
        ]

    @pl.loop(0, chunks)
    def _(c):
        for copy in copies(c):
            copy.start()

    ready()
    sums[...] = jnp.zeros_like(sums)
    capz[...] = jnp.zeros_like(capz)
    load = jnp.zeros((periods, zones), F32)
    weighted = jnp.zeros((periods, zones), F32)
    for s in range(ns):
        part = load_ref[s * periods : (s + 1) * periods, :]
        load += part * part
        weighted += level_ref[s : s + 1, 0:1] * part

    @pl.loop(0, chunks)
    def _(c):
        for copy in copies(c):
            copy.wait()
        levels = level_ref[:, 0:1]
        dual = jnp.zeros((1, tile), F32)
        caps = jnp.zeros((1, tile), F32)
        for t in range(per):
            cols = lanes(c, per * tile, t * tile, tile)
            cap = cap_ref[:, cols]
            lin = lin_ref[:, cols]
            dispatch = levels * cap
            rounded = dispatch.astype(BF16)
            on = mask_ref[c * per + t].astype(F32).astype(BF16)
            products = dot(rounded, cost[c, t], NN) + dot(rounded, coup[c, t] * on, NN)
            base = (
                (diag_ref[:, cols] + PENALTY) * dispatch + products - PENALTY * dims.mean_level * cap
            )
            base_ref[:, cols] = base
            dual += (
                periods * jnp.sum(base * base, axis=0, keepdims=True)
                + 2.0
                * jnp.sum(base, axis=0, keepdims=True)
                * jnp.sum(lin, axis=0, keepdims=True)
                + ns * jnp.sum(lin * lin, axis=0, keepdims=True)
            )
            caps += cap
            hi = cap.astype(BF16)
            rest = cap - hi.astype(F32)
            mid = rest.astype(BF16)
            low = (rest - mid.astype(F32)).astype(BF16)
            rows = jnp.concatenate(
                [jnp.broadcast_to(v.astype(F32), (8, tile)) for v in (hi, mid, low)], axis=0
            ).astype(BF16)
            capz[...] += dot(rows, zone_rows(zone_ref, cols, tile, zones), NT)
        sums[0:1, :] += dual
        sums[1:2, :] += caps

    weighted = jnp.sum(weighted, axis=0, keepdims=True) * (1.0 / dims.gen_devices)
    zcap = (capz[0:1, :] + capz[8:9, :] + capz[16:17, :]) * (1.0 / dims.scen_devices)
    dual_all = total(sums[0:1, :])
    gap_all = total(sums[1:2, :]) * float(ns * periods)
    load_all = total(load) * (1.0 / dims.gen_devices)
    ids = lax.broadcasted_iota(jnp.int32, (1, LANES), 1)
    row = jnp.where(ids == 0, gap_all, jnp.where(ids == 1, dual_all, load_all))
    parts = [row]
    for source in (zcap, weighted):
        parts += [source[:, i * LANES : (i + 1) * LANES] for i in range(zones // LANES)]
    parts.append(jnp.zeros((pack_ref.shape[1] - len(parts), LANES), F32))
    pack_ref[...] = jnp.broadcast_to(jnp.concatenate(parts, axis=0)[None], pack_ref.shape)
    return lambda: None


def scalars(dims, gap, dual, primal, size):
    target = CENTERING * gap / (2.0 * dims.entries)
    rms = jnp.sqrt(jnp.maximum(dual, 0.0) / dims.entries + EPSILON)
    primal_rms = jnp.sqrt(jnp.maximum(primal, 0.0) / dims.zone_entries + EPSILON)
    return size / (1.0 + rms), size / (1.0 + primal_rms), size * target


def keep(coef, before, k, move, shift, size):
    coef[0:8, :] = jnp.broadcast_to(move, (8, LANES))
    for i in range(k + 1):
        old = 1.0 if before is None else before[8 + 8 * i : 16 + 8 * i, :]
        coef[8 + 8 * i : 16 + 8 * i, :] = jnp.broadcast_to((1.0 - size) * old, (8, LANES))
    coef[16 + 8 * k : 24 + 8 * k, :] = jnp.broadcast_to(shift, (8, LANES))


def zone_sums(block, zone_ref, c, tot_ref):
    width, zones = block.shape[1], tot_ref.shape[1]
    tile = zones if width % zones == 0 else width
    for t in range(width // tile):
        hi, lo = split(block[:, t * tile : (t + 1) * tile])
        pick = zone_rows(zone_ref, lanes(c, width, t * tile, tile), tile, zones)
        tot_ref[...] += dot(hi, pick, NT) + dot(lo, pick, NT)


def start_body(dims, ready, first, small, large, made, large_out, scratch):
    recv_ref, size_ref, level_ref, load_ref, base_ref, lin_ref, diag_ref, cap_ref, zone_ref = small
    col_ref, price_ref, tot_ref, coef_ref = made
    (disp_ref,) = large_out
    buf, sems = scratch
    ns, periods = dims.local_scen, dims.periods
    zones = load_ref.shape[1]
    chunks, width = buf.shape[0], buf.shape[2]
    ready()
    got = jnp.sum(recv_ref[...], axis=0)
    n = zones // LANES
    zcap = jnp.concatenate([got[1 + i : 2 + i] for i in range(n)], axis=1)
    weighted = jnp.concatenate([got[1 + n + i : 2 + n + i] for i in range(n)], axis=1)
    scaled = zcap * dims.zone_scale
    primal = total(scaled * (dims.level_sq * periods * scaled - 2.0 * weighted)) + lane(got[0:1], 2)
    size = size_ref[0, 0:1, 0:1]
    move, price, shift = scalars(dims, lane(got[0:1], 0), lane(got[0:1], 1), primal, size)
    keep(coef_ref, None, 0, move, shift, size)
    for s in range(ns):
        rows = slice(s * periods, (s + 1) * periods)
        price_ref[rows, :] = price * (level_ref[s : s + 1, 0:1] * scaled - load_ref[rows, :])
    tot_ref[...] = jnp.zeros_like(tot_ref)

    @pl.loop(0, chunks)
    def _(c):
        move = coef_ref[0:1, :]
        for t in range(width // LANES):
            cols = slice(t * LANES, (t + 1) * LANES)
            here = lanes(c, width, t * LANES, LANES)
            cap, stiff, lin = cap_ref[:, here], diag_ref[:, here] + PENALTY, lin_ref[:, here]
            lowest, highest = 0.02 * cap, 0.98 * cap
            acc = jnp.zeros((periods, LANES), F32)
            dispatch = level_ref[:, 0:1] * cap
            weight = move / (stiff + 1.0 / dispatch + 1.0 / (cap - dispatch))
            base = base_ref[:, here]
            for s in range(ns):
                one = slice(s, s + 1)
                new = dispatch[one] - weight[one] * (base[one] + lin)
                new = jnp.minimum(jnp.maximum(new, lowest), highest)
                buf[c, s * periods : (s + 1) * periods, cols] = new
                acc += new
            col_ref[c * (width // LANES) + t] = acc
        pltpu.make_async_copy(buf.at[c], disp_ref.at[c], sems.at[c]).start()
        zone_sums(buf.at[c], zone_ref, c, tot_ref)

    def finish():
        @pl.loop(0, chunks)
        def _(c):
            pltpu.make_async_copy(buf.at[c], disp_ref.at[c], sems.at[c]).wait()

    return finish


def update_body(dims, k, last, ready, first, small, large, made, large_out, scratch):
    recv_ref, size_ref, coef_in, price_in, imb_ref, plan_ref, cap_ref, zone_ref = small
    if last:
        price_ref, plan_out = made
    else:
        price_ref, col_ref, tot_ref, coef_ref = made
    (disp_out,) = large_out
    disp, resid, weight, step_ref, sems, out_sems = scratch
    ns, periods = dims.local_scen, dims.periods
    chunks, width = disp.shape[0], disp.shape[2]
    moves = list(zip(large, (disp, resid, weight)))

    def in_copies(c):
        return [
            pltpu.make_async_copy(source.at[c], target.at[c], sems.at[j, c])
            for j, (source, target) in enumerate(moves)
        ]

    @pl.loop(0, chunks)
    def _(c):
        for copy in in_copies(c):
            copy.start()

    ready()
    got = jnp.sum(recv_ref[...], axis=0)
    size = size_ref[k, 0:1, 0:1]
    move, price, shift = scalars(dims, lane(got, 0), lane(got, 1), lane(got, 2), size)
    step_ref[...] = jnp.broadcast_to(move, step_ref.shape)
    price_ref[...] = price_in[...] + price * imb_ref[...]
    if last:
        for t in range(plan_ref.shape[0]):
            plan_out[:, t * LANES : (t + 1) * LANES] = plan_ref[t] * (1.0 / dims.total_scen)
    else:
        keep(coef_ref, coef_in, k, move, shift, size)
        tot_ref[...] = jnp.zeros_like(tot_ref)

    def out_copy(c):
        target = disp_out.at[:, lanes(c, width)] if last else disp_out.at[c]
        return pltpu.make_async_copy(disp.at[c], target, out_sems.at[c])

    @pl.loop(0, chunks)
    def _(c):
        for copy in in_copies(c):
            copy.wait()
        move = step_ref[0:1, :]
        for t in range(width // LANES):
            cols = slice(t * LANES, (t + 1) * LANES)
            cap = cap_ref[:, lanes(c, width, t * LANES, LANES)]
            lowest, highest = 0.02 * cap, 0.98 * cap
            pull = plan_ref[c * (width // LANES) + t] * (PENALTY / dims.total_scen)
            acc = jnp.zeros((periods, LANES), F32)
            for s in range(ns):
                rows = slice(s * periods, (s + 1) * periods)
                new = disp[c, rows, cols] - move * (resid[c, rows, cols] - pull) * weight[c, rows, cols]
                new = jnp.minimum(jnp.maximum(new, lowest), highest)
                disp[c, rows, cols] = new
                acc += new
            if not last:
                col_ref[c * (width // LANES) + t] = acc
        out_copy(c).start()
        if not last:
            zone_sums(disp.at[c], zone_ref, c, tot_ref)

    def finish():
        @pl.loop(0, chunks)
        def _(c):
            out_copy(c).wait()

    return finish


def hidden_body(dims, k, last, begin, count, ready, first, small, large, made, large_out, scratch):
    (mask_ref,) = first
    coef_ref, price_ref, part_in, lin_ref, diag_ref, cap_ref, zone_ref = small
    past, cost_in, coup_in = large[:k], large[k], large[k + 1]
    col_ref, part_ref = made
    price_hi, price_lo, sums = scratch[:3]
    disps = scratch[3 : 3 + k]
    resid, weight, cost, coup, sems, out_sems = scratch[3 + k :]
    disp = disps[-1]
    ns, periods = dims.local_scen, dims.periods
    width = disp.shape[2]
    tile, zones = cost.shape[2], price_ref.shape[1]
    per = width // tile

    moves = [(cost_in, cost), (coup_in, coup)] + list(zip(past, disps))
    outs = list(zip((resid, weight), large_out))

    def in_copies(c):
        return [
            pltpu.make_async_copy(source.at[begin + c], target.at[c], sems.at[j, c])
            for j, (source, target) in enumerate(moves)
        ]

    def out_copies(c):
        return [
            pltpu.make_async_copy(source.at[c], target.at[begin + c], out_sems.at[j, c])
            for j, (source, target) in enumerate(outs)
        ]

    @pl.loop(0, count)
    def _(c):
        for copy in in_copies(c):
            copy.start()

    ready()
    hi, lo = split(price_ref[...])
    price_hi[...] = hi
    price_lo[...] = lo
    sums[...] = jnp.zeros_like(sums)

    @pl.loop(0, count)
    def _(c):
        for copy in in_copies(c):
            copy.wait()
        kept = coef_ref[8:9, :]
        shifts = [coef_ref[16 + 8 * i : 17 + 8 * i, :] for i in range(k)]
        gap = jnp.zeros((periods, LANES), F32)
        square = jnp.zeros((periods, LANES), F32)
        for t in range(per):
            cols = slice(t * tile, (t + 1) * tile)
            hi = disp[c, :, cols].astype(BF16)
            pick = zone_rows(zone_ref, lanes(begin + c, width, t * tile, tile), tile, zones)
            on = mask_ref[(begin + c) * per + t].astype(F32).astype(BF16)
            resid[c, :, cols] = (
                dot(hi, cost[c, t], NN)
                + dot(hi, coup[c, t] * on, NN)
                + dot(price_hi[...], pick, NN)
                + dot(price_lo[...], pick, NN)
            )
            for u in range(tile // LANES):
                cols = slice(t * tile + u * LANES, t * tile + (u + 1) * LANES)
                here = lanes(begin + c, width, t * tile + u * LANES, LANES)
                cap, stiff, lin = cap_ref[:, here], diag_ref[:, here] + PENALTY, lin_ref[:, here]
                acc = jnp.zeros((periods, LANES), F32)
                for s in range(ns):
                    rows = slice(s * periods, (s + 1) * periods)
                    low, high = kept, kept
                    for shift, source in zip(shifts, disps):
                        d = source[c, rows, cols]
                        e = cap - d
                        q = 1.0 / (d * e)
                        move = shift * q
                        low = low + move * e
                        high = high + move * d
                    weight[c, rows, cols] = 1.0 / (stiff + (low * e + high * d) * q)
                    a = stiff * d + resid[c, rows, cols] + lin - low + high
                    resid[c, rows, cols] = a
                    acc += a
                    square += a * a
                    if not last:
                        gap += low * d + high * e
                col_ref[c * (width // LANES) + t * (tile // LANES) + u] = acc
        sums[0] += gap
        sums[1] += square
        for copy in out_copies(c):
            copy.start()

    ids = lax.broadcasted_iota(jnp.int32, (8, LANES), 1)
    part_ref[...] = part_in[...] + jnp.where(
        ids == 0, total(sums[0]), jnp.where(ids == 1, total(sums[1]), 0.0)
    )

    def finish():
        @pl.loop(0, count)
        def _(c):
            for copy in out_copies(c):
                copy.wait()

    return finish


def piece_kernel(recv_ref, out_ref):
    out_ref[...] = jnp.broadcast_to(jnp.sum(recv_ref[...], axis=0, keepdims=True), out_ref.shape)


def imbalance_kernel(scale, share, near_ref, far_ref, load_ref, imb_ref, part_ref):
    imb = (near_ref[...] + far_ref[...]) * scale - load_ref[...]
    imb_ref[...] = imb
    part_ref[...] = jnp.broadcast_to(total(imb * imb) * share, part_ref.shape)


def pack_body(dims, ready, first, small, large, made, large_out, scratch):
    plan_ref, part_ref, primal_ref = small[:3]
    (out_ref,) = made
    ready()
    cross = jnp.zeros(plan_ref.shape[1:], F32)
    offset = 0
    for col_ref in small[3:]:
        for t in range(col_ref.shape[0]):
            plan = plan_ref[offset + t] * (1.0 / dims.total_scen)
            cross += plan * (PENALTY * dims.local_scen * plan - 2.0 * col_ref[t])
        offset += col_ref.shape[0]
    row = part_ref[0:1, :]
    ids = lax.broadcasted_iota(jnp.int32, (1, LANES), 1)
    row = jnp.where(ids == 1, row + PENALTY * total(cross), row)
    row = jnp.where(ids == 2, primal_ref[0:1, :], row)
    out_ref[...] = jnp.broadcast_to(row[None], out_ref.shape)
    return lambda: None


class Dims:
    pass


def params(limit):
    return pltpu.CompilerParams(vmem_limit_bytes=limit << 20)


def estimate(flops, size):
    return pl.CostEstimate(flops=flops, bytes_accessed=size, transcendentals=0)


def divisor(n, most):
    return max(d for d in range(1, most + 1) if n % d == 0)


def local(
    zone_load, linear_cost, cost_diag, capacity, cost_tiles, coupling_tiles, block_map, zone_index,
    step_numer, step_denom,
):
    local_scen, periods, zones = zone_load.shape
    local_gen = capacity.shape[0]
    blocks, tile = cost_tiles.shape[0], cost_tiles.shape[2]
    iters = step_numer.shape[0]
    scen_devices, gen_devices = lax.axis_size("scen"), lax.axis_size("gen")
    devices = scen_devices * gen_devices
    rows = local_scen * periods
    gens = local_gen * gen_devices
    total_scen = local_scen * scen_devices
    all_levels = 0.2 + 0.6 * (np.arange(total_scen) + 0.5) / total_scen

    dims = Dims()
    dims.local_scen, dims.periods = local_scen, periods
    dims.scen_devices, dims.gen_devices = scen_devices, gen_devices
    dims.total_scen = total_scen
    dims.mean_level = float(all_levels.mean())
    dims.level_sq = float((all_levels**2).sum())
    dims.entries = float(total_scen * periods * gens)
    dims.zone_entries = float(total_scen * periods * zones)
    dims.zone_scale = zones / gens

    load = zone_load.reshape(rows, zones)
    diag, cap, zone = (v.reshape(1, local_gen) for v in (cost_diag, capacity, zone_index))
    mask = block_map.reshape(blocks)
    sizes = step_numer.astype(F32) / step_denom.astype(F32)
    sizes = lax.optimization_barrier(jnp.broadcast_to(sizes[:, None, None], (iters, 8, LANES)))
    scen_ids = lax.axis_index("scen") * local_scen + jnp.arange(local_scen, dtype=jnp.int32)
    levels = 0.2 + 0.6 * (scen_ids.astype(F32) + 0.5) / total_scen
    levels = jnp.broadcast_to(levels[:, None], (local_scen, LANES))

    shape = jax.ShapeDtypeStruct
    dma = pltpu.SemaphoreType.DMA

    per = divisor(blocks, 2)
    width = per * tile
    chunks = blocks // per
    lane_tiles = local_gen // LANES

    cost_c = cost_tiles.reshape(chunks, per, tile, tile)
    coup_c = coupling_tiles.reshape(chunks, per, tile, tile)
    state = shape((chunks, rows, width), F32)
    buffer = pltpu.VMEM((chunks, rows, width), F32)
    part_shape = shape((8, LANES), F32)
    plan_shape = shape((periods, local_gen), F32)
    vector = [linear_cost, diag, cap, zone]
    col_shape = shape((lane_tiles, periods, LANES), F32)
    coef_shape = shape((16 + 8 * iters, LANES), F32)
    grid_shape = shape((rows, zones), F32)

    def exchange(x):
        return lax.all_to_all(x, ("scen", "gen"), 0, 0)

    pack_rows = -(-(1 + 2 * (zones // LANES)) // 8) * 8
    tiles = pltpu.VMEM((chunks, per, tile, tile), BF16)
    base, packed = staged_call(
        functools.partial(first_body, dims), [mask], [levels, load] + vector, [cost_c, coup_c],
        [shape((local_scen, local_gen), F32), shape((devices, pack_rows, LANES), F32)], [],
        [
            pltpu.VMEM((8, tile), F32), pltpu.VMEM((24, zones), F32), tiles, tiles,
            dma((2, chunks)),
        ],
        "first",
    )
    recv = exchange(packed)

    col_sums, prices, totals, coef, dispatch = staged_call(
        functools.partial(start_body, dims), [], [recv, sizes, levels, load, base] + vector, [],
        [col_shape, grid_shape, grid_shape, coef_shape], [state], [buffer, dma((chunks,))],
        "start",
    )

    past = [dispatch]
    nothing = lax.optimization_barrier(jnp.zeros((8, LANES), F32))
    odd = lax.axis_index("gen") % 2
    pieces = col_shape.shape[0] * periods // 8
    padded = -(-pieces // scen_devices) * scen_devices
    half_rows = rows // 2
    my_load = lax.dynamic_slice_in_dim(load, odd * half_rows, half_rows, 0)
    swap = [(i, i ^ 1) for i in range(gen_devices)]
    first_half = chunks // 2
    parts = [(0, first_half), (first_half, chunks - first_half)] if first_half else [(0, chunks)]

    for k in range(1, iters):
        last = k == iters - 1
        flat = col_sums.reshape(pieces, 8, LANES)
        if padded != pieces:
            flat = jnp.pad(flat, ((0, padded - pieces), (0, 0), (0, 0)))
        flat = flat.reshape(scen_devices, padded // scen_devices, 8, LANES)
        got = lax.all_to_all(flat, "scen", 0, 0)
        other = lax.ppermute(totals, "gen", swap)

        cols = []
        resid = weight = None
        partial = nothing
        for part, (begin, count) in enumerate(parts):
            part_buffer = pltpu.VMEM((count, rows, width), F32)
            weights = pltpu.VMEM((count, per, tile, tile), BF16)
            carry = [resid, weight] if part else []
            col_k, partial, resid, weight = staged_call(
                functools.partial(hidden_body, dims, k, last, begin, count),
                [mask], [coef, prices, partial] + vector, [*past, cost_c, coup_c, *carry],
                [shape((count * width // LANES, periods, LANES), F32), part_shape], [state, state],
                [
                    pltpu.VMEM((rows, zones), BF16), pltpu.VMEM((rows, zones), BF16),
                    pltpu.VMEM((2, periods, LANES), F32),
                ] + [part_buffer] * (k + 2) + [weights, weights, dma((k + 2, count)), dma((2, count))],
                "hidden",
                estimate(count * 24 * rows * tile * tile, count * 8 * rows * width * 4),
                {k + 2 + j: j for j in range(len(carry))},
            )
            cols.append(col_k)
            if part == 0:
                got, partial = lax.optimization_barrier((got, partial))
                piece = pl.pallas_call(
                    piece_kernel, out_shape=shape(got.shape, F32), compiler_params=params(4), name="piece"
                )(got)
                piece, partial = lax.optimization_barrier((piece, partial))
                gathered = lax.all_to_all(piece, "scen", 0, 0)

                totals = totals + other
                near = lax.dynamic_slice_in_dim(totals, odd * half_rows, half_rows, 0)
                far = jnp.zeros_like(near)
                bit = 2
                while bit < gen_devices:
                    if bit > 2:
                        near = near + far
                    far = lax.ppermute(near, "gen", [(i, i ^ bit) for i in range(gen_devices)])
                    bit *= 2

        far, partial = lax.optimization_barrier((far, partial))
        plan = gathered.reshape(padded, 8, LANES)[:pieces].reshape(lane_tiles, periods, LANES)
        mine, primal = pl.pallas_call(
            functools.partial(imbalance_kernel, dims.zone_scale, 2.0 / gen_devices),
            out_shape=[shape((half_rows, zones), F32), shape((8, LANES), F32)],
            compiler_params=params(4),
            name="imbalance",
        )(near, far, my_load)
        other = lax.ppermute(mine, "gen", swap)
        imbalance = jnp.where(
            odd == 0, jnp.concatenate([mine, other]), jnp.concatenate([other, mine])
        )

        (packed,) = staged_call(
            functools.partial(pack_body, dims), [], [plan, partial, primal, *cols], [],
            [shape((devices, 1, LANES), F32)], [], [], "pack",
        )
        recv = exchange(packed)

        small = [recv, sizes, coef, prices, imbalance, plan, cap, zone]
        large = [dispatch, resid, weight]
        scratch = [buffer] * 3 + [pltpu.VMEM((8, LANES), F32), dma((3, chunks)), dma((chunks,))]
        cost = estimate(rows * local_gen * 8, rows * local_gen * 16)
        body = functools.partial(update_body, dims, k, last)
        if last:
            prices, plan, dispatch = staged_call(
                body, [], small, large, [grid_shape, plan_shape], [shape((rows, local_gen), F32)],
                scratch, "update", cost,
            )
        else:
            prices, col_sums, totals, coef, dispatch = staged_call(
                body, [], small, large, [grid_shape, col_shape, grid_shape, coef_shape], [state],
                scratch, "update", cost,
            )
            past.append(dispatch)

    return (
        dispatch.reshape(local_scen, periods, local_gen),
        prices.reshape(local_scen, periods, zones),
        plan,
    )


def solution(mesh):
    placed = (
        P("scen", None, None),
        P(None, "gen"),
        P("gen"),
        P("gen"),
        P("gen", None, None),
        P("scen", "gen", None, None),
        P("scen", "gen"),
        P("gen"),
        P(),
        P(),
    )
    return jax.shard_map(
        local,
        mesh=mesh,
        in_specs=placed,
        out_specs=(P("scen", None, "gen"), P("scen", None, None), P(None, "gen")),
        check_vma=False,
    )
```

```python
import functools

import jax
import jax.numpy as jnp
import numpy as np
from jax import lax
from jax.experimental import pallas as pl
from jax.experimental.pallas import tpu as pltpu
from jax.sharding import PartitionSpec as P

PENALTY = 2.0
CENTERING = 0.5
EPSILON = 1e-06
LANES = 128

F32 = jnp.float32
BF16 = jnp.bfloat16
NT = (((1,), (1,)), ((), ()))
NN = (((1,), (0,)), ((), ()))


def dot(a, b, dims):
    return lax.dot_general(a, b, dims, preferred_element_type=F32)


def split(x):
    hi = x.astype(BF16)
    return hi, (x - hi.astype(F32)).astype(BF16)


def lane(row, i):
    return row[:, i : i + 1]


def zone_rows(zone_ref, cols, size, zones):
    ids = lax.broadcasted_iota(jnp.int32, (zones, size), 0)
    return (ids == zone_ref[:, cols]).astype(BF16)


def total(x):
    return jnp.sum(jnp.sum(x, axis=1, keepdims=True), axis=0, keepdims=True)


def stage(body, n_near, n_small, n_large, n_small_out, n_large_out, extra):
    def kernel(*refs):
        refs = list(refs)

        def take(n):
            out = refs[:n]
            del refs[:n]
            return out

        first, near, small, large = take(extra), take(n_near), take(n_small), take(n_large)
        small_out, large_out = take(n_small_out), take(n_large_out)
        held, made = take(n_small), take(n_small_out)
        in_sems, out_sems = take(2)
        loads = [pltpu.make_async_copy(a, b, in_sems.at[j]) for j, (a, b) in enumerate(zip(small, held))]
        for copy in loads:
            copy.start()

        def ready():
            for copy in loads:
                copy.wait()

        finish = body(ready, first, near + held, large, made, large_out, refs)
        stores = [pltpu.make_async_copy(b, a, out_sems.at[j]) for j, (a, b) in enumerate(zip(small_out, made))]
        for copy in stores:
            copy.start()
        finish()
        for copy in stores:
            copy.wait()

    return kernel


def far_away(x):
    return pltpu.with_memory_space_constraint(x, pltpu.HBM)


def staged_call(
    body, first, near, small, large, small_out, large_out, scratch, name, cost=None, aliases=None,
    limit=48,
):
    dma = pltpu.SemaphoreType.DMA
    hbm = pl.BlockSpec(memory_space=pl.ANY)
    begin = len(first) + len(near) + len(small)
    held = [pltpu.VMEM(v.shape, v.dtype) for v in small + small_out]
    alias = {begin + a: len(small_out) + b for a, b in (aliases or {}).items()}
    return pl.pallas_call(
        stage(body, len(near), len(small), len(large), len(small_out), len(large_out), len(first)),
        in_specs=[pl.BlockSpec(memory_space=pltpu.SMEM)] * len(first)
        + [pl.BlockSpec(memory_space=pltpu.VMEM)] * len(near)
        + [hbm] * (len(small) + len(large)),
        out_specs=[hbm] * (len(small_out) + len(large_out)),
        out_shape=small_out + [pltpu.HBM(v.shape, v.dtype) for v in large_out],
        scratch_shapes=held
        + [dma((max(1, len(small)),)), dma((max(1, len(small_out)),))]
        + scratch,
        input_output_aliases=alias,
        compiler_params=params(limit),
        cost_estimate=cost,
        name=name,
    )(*first, *near, *small, *[far_away(v) for v in large])


def lanes(c, width, t=0, size=None):
    return pl.ds(pl.multiple_of(c * width + t, LANES), width if size is None else size)


def scen_levels(dims):
    ids = lax.broadcasted_iota(jnp.int32, (dims.local_scen, 1), 0)
    ids = ids + lax.axis_index("scen") * dims.local_scen
    return 0.2 + 0.6 * (ids.astype(F32) + 0.5) / dims.total_scen


def first_body(dims, ready, first, small, large, made, large_out, scratch):
    (mask_ref,) = first
    load_ref, lin_ref, diag_ref, cap_ref, zone_ref = small
    level = scen_levels(dims)
    cost_in, coup_in = large
    base_ref, pack_ref = made
    sums, capz, cost, coup, sems = scratch
    ns, periods = dims.local_scen, dims.periods
    zones = load_ref.shape[1]
    chunks, per, tile = cost.shape[:3]

    def copies(c):
        return [
            pltpu.make_async_copy(source.at[c], target.at[c], sems.at[j, c])
            for j, (source, target) in enumerate([(cost_in, cost), (coup_in, coup)])
        ]

    @pl.loop(0, chunks)
    def _(c):
        for copy in copies(c):
            copy.start()

    ready()
    sums[...] = jnp.zeros_like(sums)
    capz[...] = jnp.zeros_like(capz)
    load = jnp.zeros((periods, zones), F32)
    weighted = jnp.zeros((periods, zones), F32)
    for s in range(ns):
        part = load_ref[s * periods : (s + 1) * periods, :]
        load += part * part
        weighted += level[s : s + 1] * part

    @pl.loop(0, chunks)
    def _(c):
        for copy in copies(c):
            copy.wait()
        levels = scen_levels(dims)
        dual = jnp.zeros((1, tile), F32)
        caps = jnp.zeros((1, tile), F32)
        for t in range(per):
            cols = lanes(c, per * tile, t * tile, tile)
            cap = cap_ref[:, cols]
            lin = lin_ref[:, cols]
            dispatch = levels * cap
            rounded = dispatch.astype(BF16)
            on = mask_ref[c * per + t].astype(F32).astype(BF16)
            products = dot(rounded, cost[c, t], NN) + dot(rounded, coup[c, t] * on, NN)
            base = (
                (diag_ref[:, cols] + PENALTY) * dispatch + products - PENALTY * dims.mean_level * cap
            )
            base_ref[:, cols] = base

            dual += (
                periods * jnp.sum(base * base, axis=0, keepdims=True)
                + 2.0
                * jnp.sum(base, axis=0, keepdims=True)
                * jnp.sum(lin, axis=0, keepdims=True)
                + ns * jnp.sum(lin * lin, axis=0, keepdims=True)
            )
            caps += cap
            hi = cap.astype(BF16)
            rest = cap - hi.astype(F32)
            mid = rest.astype(BF16)
            low = (rest - mid.astype(F32)).astype(BF16)
            rows = jnp.concatenate(
                [jnp.broadcast_to(v.astype(F32), (8, tile)) for v in (hi, mid, low)], axis=0
            ).astype(BF16)
            capz[...] += dot(rows, zone_rows(zone_ref, cols, tile, zones), NT)
        sums[0:1, :] += dual
        sums[1:2, :] += caps

    weighted = jnp.sum(weighted, axis=0, keepdims=True) * (1.0 / dims.gen_devices)
    zcap = (capz[0:1, :] + capz[8:9, :] + capz[16:17, :]) * (1.0 / dims.scen_devices)
    dual_all = total(sums[0:1, :])
    gap_all = total(sums[1:2, :]) * float(ns * periods)
    load_all = total(load) * (1.0 / dims.gen_devices)
    ids = lax.broadcasted_iota(jnp.int32, (1, LANES), 1)
    row = jnp.where(ids == 0, gap_all, jnp.where(ids == 1, dual_all, load_all))
    parts = [row]
    for source in (zcap, weighted):
        parts += [source[:, i * LANES : (i + 1) * LANES] for i in range(zones // LANES)]
    parts.append(jnp.zeros((pack_ref.shape[1] - len(parts), LANES), F32))
    pack_ref[...] = jnp.broadcast_to(jnp.concatenate(parts, axis=0)[None], pack_ref.shape)
    return lambda: None


def scalars(dims, gap, dual, primal, size):
    target = CENTERING * gap / (2.0 * dims.entries)
    rms = jnp.sqrt(jnp.maximum(dual, 0.0) / dims.entries + EPSILON)
    primal_rms = jnp.sqrt(jnp.maximum(primal, 0.0) / dims.zone_entries + EPSILON)
    return size / (1.0 + rms), size / (1.0 + primal_rms), size * target


def keep(coef, before, k, move, shift, size):
    coef[0:8, :] = jnp.broadcast_to(move, (8, LANES))
    for i in range(k + 1):
        old = 1.0 if before is None else before[8 + 8 * i : 16 + 8 * i, :]
        coef[8 + 8 * i : 16 + 8 * i, :] = jnp.broadcast_to((1.0 - size) * old, (8, LANES))
    coef[16 + 8 * k : 24 + 8 * k, :] = jnp.broadcast_to(shift, (8, LANES))


def zone_sums(block, zone_ref, c, tot_ref):
    width, zones = block.shape[1], tot_ref.shape[1]
    tile = zones if width % zones == 0 else width
    for t in range(width // tile):
        hi, lo = split(block[:, t * tile : (t + 1) * tile])
        pick = zone_rows(zone_ref, lanes(c, width, t * tile, tile), tile, zones)
        tot_ref[...] += dot(hi, pick, NT) + dot(lo, pick, NT)


def start_body(dims, ready, first, small, large, made, large_out, scratch):
    recv_ref, size_ref, load_ref, base_ref, lin_ref, diag_ref, cap_ref, zone_ref = small
    col_ref, price_ref, tot_ref, coef_ref = made
    (disp_ref,) = large_out
    buf, sems = scratch
    level = scen_levels(dims)
    ns, periods = dims.local_scen, dims.periods
    zones = load_ref.shape[1]
    chunks, width = buf.shape[0], buf.shape[2]
    ready()
    got = jnp.sum(recv_ref[...], axis=0)
    n = zones // LANES
    zcap = jnp.concatenate([got[1 + i : 2 + i] for i in range(n)], axis=1)
    weighted = jnp.concatenate([got[1 + n + i : 2 + n + i] for i in range(n)], axis=1)
    scaled = zcap * dims.zone_scale
    primal = total(scaled * (dims.level_sq * periods * scaled - 2.0 * weighted)) + lane(got[0:1], 2)
    size = size_ref[0, 0:1, 0:1]
    move, price, shift = scalars(dims, lane(got[0:1], 0), lane(got[0:1], 1), primal, size)
    keep(coef_ref, None, 0, move, shift, size)
    for s in range(ns):
        rows = slice(s * periods, (s + 1) * periods)
        price_ref[rows, :] = price * (level[s : s + 1] * scaled - load_ref[rows, :])
    tot_ref[...] = jnp.zeros_like(tot_ref)

    @pl.loop(0, chunks)
    def _(c):
        move = coef_ref[0:1, :]
        for t in range(width // LANES):
            cols = slice(t * LANES, (t + 1) * LANES)
            here = lanes(c, width, t * LANES, LANES)
            cap, stiff, lin = cap_ref[:, here], diag_ref[:, here] + PENALTY, lin_ref[:, here]
            lowest, highest = 0.02 * cap, 0.98 * cap
            acc = jnp.zeros((periods, LANES), F32)
            dispatch = scen_levels(dims) * cap
            weight = move / (stiff + 1.0 / dispatch + 1.0 / (cap - dispatch))
            base = base_ref[:, here]
            for s in range(ns):
                one = slice(s, s + 1)
                new = dispatch[one] - weight[one] * (base[one] + lin)
                new = jnp.minimum(jnp.maximum(new, lowest), highest)
                buf[c, s * periods : (s + 1) * periods, cols] = new
                acc += new
            col_ref[c * (width // LANES) + t] = acc
        pltpu.make_async_copy(buf.at[c], disp_ref.at[c], sems.at[c]).start()
        zone_sums(buf.at[c], zone_ref, c, tot_ref)

    def finish():
        @pl.loop(0, chunks)
        def _(c):
            pltpu.make_async_copy(buf.at[c], disp_ref.at[c], sems.at[c]).wait()

    return finish


def update_body(dims, k, last, ready, first, small, large, made, large_out, scratch):
    recv_ref, imb_ref, size_ref, coef_in, price_in, plan_ref, cap_ref, zone_ref = small
    if last:
        price_ref, plan_out = made
    else:
        price_ref, col_ref, tot_ref, coef_ref = made
    (disp_out,) = large_out
    disp, resid, weight, step_ref, sems, out_sems = scratch
    ns, periods = dims.local_scen, dims.periods
    chunks, width = disp.shape[0], disp.shape[2]
    moves = list(zip(large, (disp, resid, weight)))

    def in_copies(c):
        return [
            pltpu.make_async_copy(source.at[c], target.at[c], sems.at[j, c])
            for j, (source, target) in enumerate(moves)
        ]

    @pl.loop(0, chunks)
    def _(c):
        for copy in in_copies(c):
            copy.start()

    ready()
    got = jnp.sum(recv_ref[...], axis=0)
    size = size_ref[k, 0:1, 0:1]
    move, price, shift = scalars(dims, lane(got, 0), lane(got, 1), lane(got, 2), size)
    step_ref[...] = jnp.broadcast_to(move, step_ref.shape)
    price_ref[...] = price_in[...] + price * imb_ref[...]
    if last:
        for t in range(plan_ref.shape[0]):
            plan_out[:, t * LANES : (t + 1) * LANES] = plan_ref[t] * (1.0 / dims.total_scen)
    else:
        keep(coef_ref, coef_in, k, move, shift, size)
        tot_ref[...] = jnp.zeros_like(tot_ref)

    def out_copy(c):
        target = disp_out.at[:, lanes(c, width)] if last else disp_out.at[c]
        return pltpu.make_async_copy(disp.at[c], target, out_sems.at[c])

    @pl.loop(0, chunks)
    def _(c):
        for copy in in_copies(c):
            copy.wait()
        move = step_ref[0:1, :]
        for t in range(width // LANES):
            cols = slice(t * LANES, (t + 1) * LANES)
            cap = cap_ref[:, lanes(c, width, t * LANES, LANES)]
            lowest, highest = 0.02 * cap, 0.98 * cap
            pull = plan_ref[c * (width // LANES) + t] * (PENALTY / dims.total_scen)
            acc = jnp.zeros((periods, LANES), F32)
            for s in range(ns):
                rows = slice(s * periods, (s + 1) * periods)
                new = disp[c, rows, cols] - move * (resid[c, rows, cols] - pull) * weight[c, rows, cols]
                new = jnp.minimum(jnp.maximum(new, lowest), highest)
                disp[c, rows, cols] = new
                acc += new
            if not last:
                col_ref[c * (width // LANES) + t] = acc
        out_copy(c).start()
        if not last:
            zone_sums(disp.at[c], zone_ref, c, tot_ref)

    def finish():
        @pl.loop(0, chunks)
        def _(c):
            out_copy(c).wait()

    return finish


def hidden_body(dims, k, last, begin, count, ready, first, small, large, made, large_out, scratch):
    (mask_ref,) = first
    coef_ref, price_ref, part_in, lin_ref, diag_ref, cap_ref, zone_ref = small
    past, cost_in, coup_in = large[:k], large[k], large[k + 1]
    col_ref, part_ref = made
    price_hi, price_lo, sums = scratch[:3]
    disps = scratch[3 : 3 + k]
    resid, weight, cost, coup, sems, out_sems = scratch[3 + k :]
    disp = disps[-1]
    ns, periods = dims.local_scen, dims.periods
    width = disp.shape[2]
    tile, zones = cost.shape[2], price_ref.shape[1]
    per = width // tile

    moves = [(cost_in, cost), (coup_in, coup)] + list(zip(past, disps))
    outs = list(zip((resid, weight), large_out))

    def in_copies(c):
        return [
            pltpu.make_async_copy(source.at[begin + c], target.at[c], sems.at[j, c])
            for j, (source, target) in enumerate(moves)
        ]

    def out_copies(c):
        return [
            pltpu.make_async_copy(source.at[c], target.at[begin + c], out_sems.at[j, c])
            for j, (source, target) in enumerate(outs)
        ]

    @pl.loop(0, count)
    def _(c):
        for copy in in_copies(c):
            copy.start()

    ready()
    hi, lo = split(price_ref[...])
    price_hi[...] = hi
    price_lo[...] = lo
    sums[...] = jnp.zeros_like(sums)

    @pl.loop(0, count)
    def _(c):
        for copy in in_copies(c):
            copy.wait()
        kept = coef_ref[8:9, :]
        shifts = [coef_ref[16 + 8 * i : 17 + 8 * i, :] for i in range(k)]
        gap = jnp.zeros((periods, LANES), F32)
        square = jnp.zeros((periods, LANES), F32)
        for t in range(per):
            cols = slice(t * tile, (t + 1) * tile)
            hi = disp[c, :, cols].astype(BF16)
            pick = zone_rows(zone_ref, lanes(begin + c, width, t * tile, tile), tile, zones)
            on = mask_ref[(begin + c) * per + t].astype(F32).astype(BF16)
            resid[c, :, cols] = (
                dot(hi, cost[c, t], NN)
                + dot(hi, coup[c, t] * on, NN)
                + dot(price_hi[...], pick, NN)
                + dot(price_lo[...], pick, NN)
            )
            for u in range(tile // LANES):
                cols = slice(t * tile + u * LANES, t * tile + (u + 1) * LANES)
                here = lanes(begin + c, width, t * tile + u * LANES, LANES)
                cap, stiff, lin = cap_ref[:, here], diag_ref[:, here] + PENALTY, lin_ref[:, here]
                acc = jnp.zeros((periods, LANES), F32)
                for s in range(ns):
                    rows = slice(s * periods, (s + 1) * periods)
                    low, high = kept, kept
                    for shift, source in zip(shifts, disps):
                        d = source[c, rows, cols]
                        e = cap - d
                        q = 1.0 / (d * e)
                        move = shift * q
                        low = low + move * e
                        high = high + move * d
                    weight[c, rows, cols] = 1.0 / (stiff + (low * e + high * d) * q)
                    a = stiff * d + resid[c, rows, cols] + lin - low + high
                    resid[c, rows, cols] = a
                    acc += a
                    square += a * a
                    if not last:
                        gap += low * d + high * e
                col_ref[c * (width // LANES) + t * (tile // LANES) + u] = acc
        sums[0] += gap
        sums[1] += square
        for copy in out_copies(c):
            copy.start()

    ids = lax.broadcasted_iota(jnp.int32, (8, LANES), 1)
    part_ref[...] = part_in[...] + jnp.where(
        ids == 0, total(sums[0]), jnp.where(ids == 1, total(sums[1]), 0.0)
    )

    def finish():
        @pl.loop(0, count)
        def _(c):
            for copy in out_copies(c):
                copy.wait()

    return finish


def piece_kernel(recv_ref, out_ref):
    out_ref[...] = jnp.broadcast_to(jnp.sum(recv_ref[...], axis=0, keepdims=True), out_ref.shape)


def imbalance_kernel(scale, share, near_ref, far_ref, load_ref, imb_ref, part_ref):
    imb = (near_ref[...] + far_ref[...]) * scale - load_ref[...]
    imb_ref[...] = imb
    part_ref[...] = jnp.broadcast_to(total(imb * imb) * share, part_ref.shape)


def pack_body(dims, ready, first, small, large, made, large_out, scratch):
    plan_ref, primal_ref, part_ref = small[:3]
    (out_ref,) = made
    ready()
    cross = jnp.zeros(plan_ref.shape[1:], F32)
    offset = 0
    for col_ref in small[3:]:
        for t in range(col_ref.shape[0]):
            plan = plan_ref[offset + t] * (1.0 / dims.total_scen)
            cross += plan * (PENALTY * dims.local_scen * plan - 2.0 * col_ref[t])
        offset += col_ref.shape[0]
    row = part_ref[0:1, :]
    ids = lax.broadcasted_iota(jnp.int32, (1, LANES), 1)
    row = jnp.where(ids == 1, row + PENALTY * total(cross), row)
    row = jnp.where(ids == 2, primal_ref[0:1, :], row)
    out_ref[...] = jnp.broadcast_to(row[None], out_ref.shape)
    return lambda: None


class Dims:
    pass


def params(limit):
    return pltpu.CompilerParams(vmem_limit_bytes=limit << 20)


def estimate(flops, size):
    return pl.CostEstimate(flops=flops, bytes_accessed=size, transcendentals=0)


def divisor(n, most):
    return max(d for d in range(1, most + 1) if n % d == 0)


def local(
    zone_load, linear_cost, cost_diag, capacity, cost_tiles, coupling_tiles, block_map, zone_index,
    step_numer, step_denom,
):
    local_scen, periods, zones = zone_load.shape
    local_gen = capacity.shape[0]
    blocks, tile = cost_tiles.shape[0], cost_tiles.shape[2]
    iters = step_numer.shape[0]
    scen_devices, gen_devices = lax.axis_size("scen"), lax.axis_size("gen")
    devices = scen_devices * gen_devices
    rows = local_scen * periods
    gens = local_gen * gen_devices
    total_scen = local_scen * scen_devices
    all_levels = 0.2 + 0.6 * (np.arange(total_scen) + 0.5) / total_scen

    dims = Dims()
    dims.local_scen, dims.periods = local_scen, periods
    dims.scen_devices, dims.gen_devices = scen_devices, gen_devices
    dims.total_scen = total_scen
    dims.mean_level = float(all_levels.mean())
    dims.level_sq = float((all_levels**2).sum())
    dims.entries = float(total_scen * periods * gens)
    dims.zone_entries = float(total_scen * periods * zones)
    dims.zone_scale = zones / gens

    load = zone_load.reshape(rows, zones)
    diag, cap, zone = (v.reshape(1, local_gen) for v in (cost_diag, capacity, zone_index))
    mask = block_map.reshape(blocks)
    sizes = step_numer.astype(F32) / step_denom.astype(F32)
    sizes = lax.optimization_barrier(jnp.broadcast_to(sizes[:, None, None], (iters, 8, LANES)))

    shape = jax.ShapeDtypeStruct
    dma = pltpu.SemaphoreType.DMA

    per = divisor(blocks, 2)
    width = per * tile
    chunks = blocks // per
    lane_tiles = local_gen // LANES

    cost_c = cost_tiles.reshape(chunks, per, tile, tile)
    coup_c = coupling_tiles.reshape(chunks, per, tile, tile)
    state = shape((chunks, rows, width), F32)
    buffer = pltpu.VMEM((chunks, rows, width), F32)
    part_shape = shape((8, LANES), F32)
    plan_shape = shape((periods, local_gen), F32)
    vector = [linear_cost, diag, cap, zone]
    col_shape = shape((lane_tiles, periods, LANES), F32)
    coef_shape = shape((16 + 8 * iters, LANES), F32)
    grid_shape = shape((rows, zones), F32)

    def exchange(x):
        return lax.all_to_all(x, ("scen", "gen"), 0, 0)

    pack_rows = -(-(1 + 2 * (zones // LANES)) // 8) * 8
    tiles = pltpu.VMEM((chunks, per, tile, tile), BF16)
    base, packed = staged_call(
        functools.partial(first_body, dims), [mask], [], [load] + vector, [cost_c, coup_c],
        [shape((local_scen, local_gen), F32), shape((devices, pack_rows, LANES), F32)], [],
        [
            pltpu.VMEM((8, tile), F32), pltpu.VMEM((24, zones), F32), tiles, tiles,
            dma((2, chunks)),
        ],
        "first", limit=60,
    )
    recv = exchange(packed)

    col_sums, prices, totals, coef, dispatch = staged_call(
        functools.partial(start_body, dims), [], [recv], [sizes, load, base] + vector, [],
        [col_shape, grid_shape, grid_shape, coef_shape], [state], [buffer, dma((chunks,))],
        "start",
    )

    past = [dispatch]
    nothing = lax.optimization_barrier(jnp.zeros((8, LANES), F32))
    odd = lax.axis_index("gen") % 2
    pieces = col_shape.shape[0] * periods // 8
    padded = -(-pieces // scen_devices) * scen_devices
    half_rows = rows // 2
    my_load = lax.dynamic_slice_in_dim(load, odd * half_rows, half_rows, 0)
    swap = [(i, i ^ 1) for i in range(gen_devices)]
    first_half = chunks // 2
    parts = [(0, first_half), (first_half, chunks - first_half)] if first_half else [(0, chunks)]

    for k in range(1, iters):
        last = k == iters - 1
        flat = col_sums.reshape(pieces, 8, LANES)
        if padded != pieces:
            flat = jnp.pad(flat, ((0, padded - pieces), (0, 0), (0, 0)))
        flat = flat.reshape(scen_devices, padded // scen_devices, 8, LANES)
        got = lax.all_to_all(flat, "scen", 0, 0)
        other = lax.ppermute(totals, "gen", swap)

        cols = []
        resid = weight = None
        partial = nothing
        for part, (begin, count) in enumerate(parts):
            part_buffer = pltpu.VMEM((count, rows, width), F32)
            weights = pltpu.VMEM((count, per, tile, tile), BF16)
            carry = [resid, weight] if part else []
            col_k, partial, resid, weight = staged_call(
                functools.partial(hidden_body, dims, k, last, begin, count),
                [mask], [], [coef, prices, partial] + vector, [*past, cost_c, coup_c, *carry],
                [shape((count * width // LANES, periods, LANES), F32), part_shape], [state, state],
                [
                    pltpu.VMEM((rows, zones), BF16), pltpu.VMEM((rows, zones), BF16),
                    pltpu.VMEM((2, periods, LANES), F32),
                ] + [part_buffer] * (k + 2) + [weights, weights, dma((k + 2, count)), dma((2, count))],
                "hidden",
                estimate(count * 24 * rows * tile * tile, count * 8 * rows * width * 4),
                {k + 2 + j: j for j in range(len(carry))},
            )
            cols.append(col_k)
            if part == 0:
                got, partial = lax.optimization_barrier((got, partial))
                piece = pl.pallas_call(
                    piece_kernel, out_shape=shape(got.shape, F32), compiler_params=params(4), name="piece"
                )(got)
                piece, partial = lax.optimization_barrier((piece, partial))
                gathered = lax.all_to_all(piece, "scen", 0, 0)

                totals = totals + other
                near = lax.dynamic_slice_in_dim(totals, odd * half_rows, half_rows, 0)
                far = jnp.zeros_like(near)
                bit = 2
                while bit < gen_devices:
                    if bit > 2:
                        near = near + far
                    far = lax.ppermute(near, "gen", [(i, i ^ bit) for i in range(gen_devices)])
                    bit *= 2

        far, partial = lax.optimization_barrier((far, partial))
        plan = gathered.reshape(padded, 8, LANES)[:pieces].reshape(lane_tiles, periods, LANES)
        mine, primal = pl.pallas_call(
            functools.partial(imbalance_kernel, dims.zone_scale, 2.0 / gen_devices),
            out_shape=[shape((half_rows, zones), F32), shape((8, LANES), F32)],
            compiler_params=params(4),
            name="imbalance",
        )(near, far, my_load)
        other = lax.ppermute(mine, "gen", swap)
        imbalance = jnp.where(
            odd == 0, jnp.concatenate([mine, other]), jnp.concatenate([other, mine])
        )

        (packed,) = staged_call(
            functools.partial(pack_body, dims), [], [plan, primal, partial], [far_away(v) for v in cols], [],
            [shape((devices, 1, LANES), F32)], [], [], "pack", limit=4,
        )
        recv = exchange(packed)

        near, small = [recv], [imbalance, sizes, coef, prices, plan, cap, zone]
        large = [dispatch, resid, weight]
        scratch = [buffer] * 3 + [pltpu.VMEM((8, LANES), F32), dma((3, chunks)), dma((chunks,))]
        cost = estimate(rows * local_gen * 8, rows * local_gen * 16)
        body = functools.partial(update_body, dims, k, last)
        if last:
            prices, plan, dispatch = staged_call(
                body, [], near, small, large, [grid_shape, plan_shape], [shape((rows, local_gen), F32)],
                scratch, "update", cost,
            )
        else:
            prices, col_sums, totals, coef, dispatch = staged_call(
                body, [], near, small, large, [grid_shape, col_shape, grid_shape, coef_shape], [state],
                scratch, "update", cost,
            )
            past.append(dispatch)

    return (
        dispatch.reshape(local_scen, periods, local_gen),
        prices.reshape(local_scen, periods, zones),
        plan,
    )


def solution(mesh):
    placed = (
        P("scen", None, None),
        P(None, "gen"),
        P("gen"),
        P("gen"),
        P("gen", None, None),
        P("scen", "gen", None, None),
        P("scen", "gen"),
        P("gen"),
        P(),
        P(),
    )
    return jax.shard_map(
        local,
        mesh=mesh,
        in_specs=placed,
        out_specs=(P("scen", None, "gen"), P("scen", None, None), P(None, "gen")),
        check_vma=False,
    )
```

```python
import functools

import jax
import jax.numpy as jnp
import numpy as np
from jax import lax
from jax.experimental import pallas as pl
from jax.experimental.pallas import tpu as pltpu
from jax.sharding import PartitionSpec as P

PENALTY = 2.0
CENTERING = 0.5
EPSILON = 1e-06
LANES = 128

F32 = jnp.float32
BF16 = jnp.bfloat16
NT = (((1,), (1,)), ((), ()))
NN = (((1,), (0,)), ((), ()))


def dot(a, b, dims):
    return lax.dot_general(a, b, dims, preferred_element_type=F32)


def split(x):
    hi = x.astype(BF16)
    return hi, (x - hi.astype(F32)).astype(BF16)


def lane(row, i):
    return row[:, i : i + 1]


def zone_rows(zone_ref, cols, size, zones):
    ids = lax.broadcasted_iota(jnp.int32, (zones, size), 0)
    return (ids == zone_ref[:, cols]).astype(BF16)


def total(x):
    return jnp.sum(jnp.sum(x, axis=1, keepdims=True), axis=0, keepdims=True)


def stage(body, n_near, n_small, n_large, n_small_out, n_large_out, extra):
    def kernel(*refs):
        refs = list(refs)

        def take(n):
            out = refs[:n]
            del refs[:n]
            return out

        first, near, small, large = take(extra), take(n_near), take(n_small), take(n_large)
        small_out, large_out = take(n_small_out), take(n_large_out)
        held, made = take(n_small), take(n_small_out)
        in_sems, out_sems = take(2)
        loads = [pltpu.make_async_copy(a, b, in_sems.at[j]) for j, (a, b) in enumerate(zip(small, held))]
        for copy in loads:
            copy.start()

        def ready():
            for copy in loads:
                copy.wait()

        finish = body(ready, first, near + held, large, made, large_out, refs)
        stores = [pltpu.make_async_copy(b, a, out_sems.at[j]) for j, (a, b) in enumerate(zip(small_out, made))]
        for copy in stores:
            copy.start()
        finish()
        for copy in stores:
            copy.wait()

    return kernel


def far_away(x):
    return pltpu.with_memory_space_constraint(x, pltpu.HBM)


def staged_call(
    body, first, near, small, large, small_out, large_out, scratch, name, cost=None, aliases=None,
    limit=48,
):
    dma = pltpu.SemaphoreType.DMA
    hbm = pl.BlockSpec(memory_space=pl.ANY)
    begin = len(first) + len(near) + len(small)
    held = [pltpu.VMEM(v.shape, v.dtype) for v in small + small_out]
    alias = {begin + a: len(small_out) + b for a, b in (aliases or {}).items()}
    return pl.pallas_call(
        stage(body, len(near), len(small), len(large), len(small_out), len(large_out), len(first)),
        in_specs=[pl.BlockSpec(memory_space=pltpu.SMEM)] * len(first)
        + [pl.BlockSpec(memory_space=pltpu.VMEM)] * len(near)
        + [hbm] * (len(small) + len(large)),
        out_specs=[hbm] * (len(small_out) + len(large_out)),
        out_shape=small_out + [pltpu.HBM(v.shape, v.dtype) for v in large_out],
        scratch_shapes=held
        + [dma((max(1, len(small)),)), dma((max(1, len(small_out)),))]
        + scratch,
        input_output_aliases=alias,
        compiler_params=params(limit),
        cost_estimate=cost,
        name=name,
    )(*first, *near, *small, *[far_away(v) for v in large])


def lanes(c, width, t=0, size=None):
    return pl.ds(pl.multiple_of(c * width + t, LANES), width if size is None else size)


def scen_levels(dims):
    ids = lax.broadcasted_iota(jnp.int32, (dims.local_scen, 1), 0)
    ids = ids + lax.axis_index("scen") * dims.local_scen
    return 0.2 + 0.6 * (ids.astype(F32) + 0.5) / dims.total_scen


def first_body(dims, ready, first, small, large, made, large_out, scratch):
    (mask_ref,) = first
    load_ref, lin_ref, diag_ref, cap_ref, zone_ref = small
    level = scen_levels(dims)
    cost_in, coup_in = large
    base_ref, pack_ref = made
    sums, capz, cost, coup, sems = scratch
    ns, periods = dims.local_scen, dims.periods
    zones = load_ref.shape[1]
    chunks, per, tile = cost.shape[:3]

    def copies(c):
        return [
            pltpu.make_async_copy(source.at[c], target.at[c], sems.at[j, c])
            for j, (source, target) in enumerate([(cost_in, cost), (coup_in, coup)])
        ]

    @pl.loop(0, chunks)
    def _(c):
        for copy in copies(c):
            copy.start()

    ready()
    sums[...] = jnp.zeros_like(sums)
    capz[...] = jnp.zeros_like(capz)
    load = jnp.zeros((periods, zones), F32)
    weighted = jnp.zeros((periods, zones), F32)
    for s in range(ns):
        part = load_ref[s * periods : (s + 1) * periods, :]
        load += part * part
        weighted += level[s : s + 1] * part

    @pl.loop(0, chunks)
    def _(c):
        for copy in copies(c):
            copy.wait()
        levels = scen_levels(dims)
        dual = jnp.zeros((1, tile), F32)
        caps = jnp.zeros((1, tile), F32)
        for t in range(per):
            cols = lanes(c, per * tile, t * tile, tile)
            cap = cap_ref[:, cols]
            lin = lin_ref[:, cols]
            dispatch = levels * cap
            rounded = dispatch.astype(BF16)
            on = mask_ref[c * per + t].astype(F32).astype(BF16)
            products = dot(rounded, cost[c, t], NN) + dot(rounded, coup[c, t] * on, NN)
            base = (
                (diag_ref[:, cols] + PENALTY) * dispatch + products - PENALTY * dims.mean_level * cap
            )
            base_ref[:, cols] = base

            dual += (
                periods * jnp.sum(base * base, axis=0, keepdims=True)
                + 2.0
                * jnp.sum(base, axis=0, keepdims=True)
                * jnp.sum(lin, axis=0, keepdims=True)
                + ns * jnp.sum(lin * lin, axis=0, keepdims=True)
            )
            caps += cap
            hi = cap.astype(BF16)
            rest = cap - hi.astype(F32)
            mid = rest.astype(BF16)
            low = (rest - mid.astype(F32)).astype(BF16)
            rows = jnp.concatenate(
                [jnp.broadcast_to(v.astype(F32), (8, tile)) for v in (hi, mid, low)], axis=0
            ).astype(BF16)
            capz[...] += dot(rows, zone_rows(zone_ref, cols, tile, zones), NT)
        sums[0:1, :] += dual
        sums[1:2, :] += caps

    weighted = jnp.sum(weighted, axis=0, keepdims=True) * (1.0 / dims.gen_devices)
    zcap = (capz[0:1, :] + capz[8:9, :] + capz[16:17, :]) * (1.0 / dims.scen_devices)
    dual_all = total(sums[0:1, :])
    gap_all = total(sums[1:2, :]) * float(ns * periods)
    load_all = total(load) * (1.0 / dims.gen_devices)
    ids = lax.broadcasted_iota(jnp.int32, (1, LANES), 1)
    row = jnp.where(ids == 0, gap_all, jnp.where(ids == 1, dual_all, load_all))
    parts = [row]
    for source in (zcap, weighted):
        parts += [source[:, i * LANES : (i + 1) * LANES] for i in range(zones // LANES)]
    parts.append(jnp.zeros((pack_ref.shape[1] - len(parts), LANES), F32))
    pack_ref[...] = jnp.broadcast_to(jnp.concatenate(parts, axis=0)[None], pack_ref.shape)
    return lambda: None


def scalars(dims, gap, dual, primal, size):
    target = CENTERING * gap / (2.0 * dims.entries)
    rms = jnp.sqrt(jnp.maximum(dual, 0.0) / dims.entries + EPSILON)
    primal_rms = jnp.sqrt(jnp.maximum(primal, 0.0) / dims.zone_entries + EPSILON)
    return size / (1.0 + rms), size / (1.0 + primal_rms), size * target


def keep(coef, before, k, move, shift, size):
    coef[0:8, :] = jnp.broadcast_to(move, (8, LANES))
    for i in range(k + 1):
        old = 1.0 if before is None else before[8 + 8 * i : 16 + 8 * i, :]
        coef[8 + 8 * i : 16 + 8 * i, :] = jnp.broadcast_to((1.0 - size) * old, (8, LANES))
    coef[16 + 8 * k : 24 + 8 * k, :] = jnp.broadcast_to(shift, (8, LANES))


def zone_sums(block, zone_ref, c, tot_ref):
    width, zones = block.shape[1], tot_ref.shape[1]
    tile = zones if width % zones == 0 else width
    for t in range(width // tile):
        hi, lo = split(block[:, t * tile : (t + 1) * tile])
        pick = zone_rows(zone_ref, lanes(c, width, t * tile, tile), tile, zones)
        tot_ref[...] += dot(hi, pick, NT) + dot(lo, pick, NT)


def start_body(dims, ready, first, small, large, made, large_out, scratch):
    recv_ref, size_ref, load_ref, base_ref, lin_ref, diag_ref, cap_ref, zone_ref = small
    col_ref, price_ref, tot_ref, coef_ref = made
    (disp_ref,) = large_out
    buf, sems = scratch
    level = scen_levels(dims)
    ns, periods = dims.local_scen, dims.periods
    zones = load_ref.shape[1]
    chunks, width = buf.shape[0], buf.shape[2]
    ready()
    got = jnp.sum(recv_ref[...], axis=0)
    n = zones // LANES
    zcap = jnp.concatenate([got[1 + i : 2 + i] for i in range(n)], axis=1)
    weighted = jnp.concatenate([got[1 + n + i : 2 + n + i] for i in range(n)], axis=1)
    scaled = zcap * dims.zone_scale
    primal = total(scaled * (dims.level_sq * periods * scaled - 2.0 * weighted)) + lane(got[0:1], 2)
    size = size_ref[0, 0:1, 0:1]
    move, price, shift = scalars(dims, lane(got[0:1], 0), lane(got[0:1], 1), primal, size)
    keep(coef_ref, None, 0, move, shift, size)
    for s in range(ns):
        rows = slice(s * periods, (s + 1) * periods)
        price_ref[rows, :] = price * (level[s : s + 1] * scaled - load_ref[rows, :])
    tot_ref[...] = jnp.zeros_like(tot_ref)

    @pl.loop(0, chunks)
    def _(c):
        move = coef_ref[0:1, :]
        for t in range(width // LANES):
            cols = slice(t * LANES, (t + 1) * LANES)
            here = lanes(c, width, t * LANES, LANES)
            cap, stiff, lin = cap_ref[:, here], diag_ref[:, here] + PENALTY, lin_ref[:, here]
            lowest, highest = 0.02 * cap, 0.98 * cap
            acc = jnp.zeros((periods, LANES), F32)
            dispatch = scen_levels(dims) * cap
            weight = move / (stiff + 1.0 / dispatch + 1.0 / (cap - dispatch))
            base = base_ref[:, here]
            for s in range(ns):
                one = slice(s, s + 1)
                new = dispatch[one] - weight[one] * (base[one] + lin)
                new = jnp.minimum(jnp.maximum(new, lowest), highest)
                buf[c, s * periods : (s + 1) * periods, cols] = new
                acc += new
            col_ref[c * (width // LANES) + t] = acc
        pltpu.make_async_copy(buf.at[c], disp_ref.at[c], sems.at[c]).start()
        zone_sums(buf.at[c], zone_ref, c, tot_ref)

    def finish():
        @pl.loop(0, chunks)
        def _(c):
            pltpu.make_async_copy(buf.at[c], disp_ref.at[c], sems.at[c]).wait()

    return finish


def update_body(dims, k, last, ready, first, small, large, made, large_out, scratch):
    recv_ref, imb_ref, size_ref, coef_in, price_in, plan_ref, cap_ref, zone_ref = small
    if last:
        price_ref, plan_out = made
    else:
        price_ref, col_ref, tot_ref, coef_ref = made
    (disp_out,) = large_out
    disp, resid, weight, step_ref, sems, out_sems = scratch
    ns, periods = dims.local_scen, dims.periods
    chunks, width = disp.shape[0], disp.shape[2]
    moves = list(zip(large, (disp, resid, weight)))

    def in_copies(c):
        return [
            pltpu.make_async_copy(source.at[c], target.at[c], sems.at[j, c])
            for j, (source, target) in enumerate(moves)
        ]

    @pl.loop(0, chunks)
    def _(c):
        for copy in in_copies(c):
            copy.start()

    ready()
    got = jnp.sum(recv_ref[...], axis=0)
    size = size_ref[k, 0:1, 0:1]
    move, price, shift = scalars(dims, lane(got, 0), lane(got, 1), lane(got, 2), size)
    step_ref[...] = jnp.broadcast_to(move, step_ref.shape)
    price_ref[...] = price_in[...] + price * imb_ref[...]
    if last:
        for t in range(plan_ref.shape[0]):
            plan_out[:, t * LANES : (t + 1) * LANES] = plan_ref[t] * (1.0 / dims.total_scen)
    else:
        keep(coef_ref, coef_in, k, move, shift, size)
        tot_ref[...] = jnp.zeros_like(tot_ref)

    def out_copy(c):
        target = disp_out.at[:, lanes(c, width)] if last else disp_out.at[c]
        return pltpu.make_async_copy(disp.at[c], target, out_sems.at[c])

    @pl.loop(0, chunks)
    def _(c):
        for copy in in_copies(c):
            copy.wait()
        move = step_ref[0:1, :]
        for t in range(width // LANES):
            cols = slice(t * LANES, (t + 1) * LANES)
            cap = cap_ref[:, lanes(c, width, t * LANES, LANES)]
            lowest, highest = 0.02 * cap, 0.98 * cap
            pull = plan_ref[c * (width // LANES) + t] * (PENALTY / dims.total_scen)
            acc = jnp.zeros((periods, LANES), F32)
            for s in range(ns):
                rows = slice(s * periods, (s + 1) * periods)
                new = disp[c, rows, cols] - move * (resid[c, rows, cols] - pull) * weight[c, rows, cols]
                new = jnp.minimum(jnp.maximum(new, lowest), highest)
                disp[c, rows, cols] = new
                acc += new
            if not last:
                col_ref[c * (width // LANES) + t] = acc
        out_copy(c).start()
        if not last:
            zone_sums(disp.at[c], zone_ref, c, tot_ref)

    def finish():
        @pl.loop(0, chunks)
        def _(c):
            out_copy(c).wait()

    return finish


def hidden_body(dims, k, last, begin, count, ready, first, small, large, made, large_out, scratch):
    (mask_ref,) = first
    coef_ref, price_ref, part_in, lin_ref, diag_ref, cap_ref, zone_ref = small
    past, cost_in, coup_in = large[:k], large[k], large[k + 1]
    col_ref, part_ref = made
    price_hi, price_lo, sums = scratch[:3]
    disps = scratch[3 : 3 + k]
    resid, weight, cost, coup, sems, out_sems = scratch[3 + k :]
    disp = disps[-1]
    ns, periods = dims.local_scen, dims.periods
    width = disp.shape[2]
    tile, zones = cost.shape[2], price_ref.shape[1]
    per = width // tile

    moves = [(cost_in, cost), (coup_in, coup)] + list(zip(past, disps))
    outs = list(zip((resid, weight), large_out))

    def in_copies(c):
        return [
            pltpu.make_async_copy(source.at[begin + c], target.at[c], sems.at[j, c])
            for j, (source, target) in enumerate(moves)
        ]

    def out_copies(c):
        return [
            pltpu.make_async_copy(source.at[c], target.at[begin + c], out_sems.at[j, c])
            for j, (source, target) in enumerate(outs)
        ]

    @pl.loop(0, count)
    def _(c):
        for copy in in_copies(c):
            copy.start()

    ready()
    hi, lo = split(price_ref[...])
    price_hi[...] = hi
    price_lo[...] = lo
    sums[...] = jnp.zeros_like(sums)

    @pl.loop(0, count)
    def _(c):
        for copy in in_copies(c):
            copy.wait()
        kept = coef_ref[8:9, :]
        shifts = [coef_ref[16 + 8 * i : 17 + 8 * i, :] for i in range(k)]
        gap = jnp.zeros((periods, LANES), F32)
        square = jnp.zeros((periods, LANES), F32)
        for t in range(per):
            cols = slice(t * tile, (t + 1) * tile)
            hi = disp[c, :, cols].astype(BF16)
            pick = zone_rows(zone_ref, lanes(begin + c, width, t * tile, tile), tile, zones)
            on = mask_ref[(begin + c) * per + t].astype(F32).astype(BF16)
            resid[c, :, cols] = (
                dot(hi, cost[c, t], NN)
                + dot(hi, coup[c, t] * on, NN)
                + dot(price_hi[...], pick, NN)
                + dot(price_lo[...], pick, NN)
            )
            for u in range(tile // LANES):
                cols = slice(t * tile + u * LANES, t * tile + (u + 1) * LANES)
                here = lanes(begin + c, width, t * tile + u * LANES, LANES)
                cap, stiff, lin = cap_ref[:, here], diag_ref[:, here] + PENALTY, lin_ref[:, here]
                acc = jnp.zeros((periods, LANES), F32)
                for s in range(ns):
                    rows = slice(s * periods, (s + 1) * periods)
                    low, high = kept, kept
                    for shift, source in zip(shifts, disps):
                        d = source[c, rows, cols]
                        e = cap - d
                        q = 1.0 / (d * e)
                        move = shift * q
                        low = low + move * e
                        high = high + move * d
                    weight[c, rows, cols] = 1.0 / (stiff + (low * e + high * d) * q)
                    a = stiff * d + resid[c, rows, cols] + lin - low + high
                    resid[c, rows, cols] = a
                    acc += a
                    square += a * a
                    if not last:
                        gap += low * d + high * e
                col_ref[c * (width // LANES) + t * (tile // LANES) + u] = acc
        sums[0] += gap
        sums[1] += square
        for copy in out_copies(c):
            copy.start()

    ids = lax.broadcasted_iota(jnp.int32, (8, LANES), 1)
    part_ref[...] = part_in[...] + jnp.where(
        ids == 0, total(sums[0]), jnp.where(ids == 1, total(sums[1]), 0.0)
    )

    def finish():
        @pl.loop(0, count)
        def _(c):
            for copy in out_copies(c):
                copy.wait()

    return finish


def piece_kernel(recv_ref, out_ref):
    out_ref[...] = jnp.broadcast_to(jnp.sum(recv_ref[...], axis=0, keepdims=True), out_ref.shape)


def imbalance_kernel(scale, share, near_ref, far_ref, load_ref, imb_ref, part_ref):
    imb = (near_ref[...] + far_ref[...]) * scale - load_ref[...]
    imb_ref[...] = imb
    part_ref[...] = jnp.broadcast_to(total(imb * imb) * share, part_ref.shape)


def pack_body(dims, ready, first, small, large, made, large_out, scratch):
    plan_ref, primal_ref, part_ref = small[:3]
    (out_ref,) = made
    ready()
    cross = jnp.zeros(plan_ref.shape[1:], F32)
    offset = 0
    for col_ref in small[3:]:
        for t in range(col_ref.shape[0]):
            plan = plan_ref[offset + t] * (1.0 / dims.total_scen)
            cross += plan * (PENALTY * dims.local_scen * plan - 2.0 * col_ref[t])
        offset += col_ref.shape[0]
    row = part_ref[0:1, :]
    ids = lax.broadcasted_iota(jnp.int32, (1, LANES), 1)
    row = jnp.where(ids == 1, row + PENALTY * total(cross), row)
    row = jnp.where(ids == 2, primal_ref[0:1, :], row)
    out_ref[...] = jnp.broadcast_to(row[None], out_ref.shape)
    return lambda: None


class Dims:
    pass


def params(limit):
    return pltpu.CompilerParams(vmem_limit_bytes=limit << 20)


def estimate(flops, size):
    return pl.CostEstimate(flops=flops, bytes_accessed=size, transcendentals=0)


def divisor(n, most):
    return max(d for d in range(1, most + 1) if n % d == 0)


def local(
    zone_load, linear_cost, cost_diag, capacity, cost_tiles, coupling_tiles, block_map, zone_index,
    step_numer, step_denom,
):
    local_scen, periods, zones = zone_load.shape
    local_gen = capacity.shape[0]
    blocks, tile = cost_tiles.shape[0], cost_tiles.shape[2]
    iters = step_numer.shape[0]
    scen_devices, gen_devices = lax.axis_size("scen"), lax.axis_size("gen")
    devices = scen_devices * gen_devices
    rows = local_scen * periods
    gens = local_gen * gen_devices
    total_scen = local_scen * scen_devices
    all_levels = 0.2 + 0.6 * (np.arange(total_scen) + 0.5) / total_scen

    dims = Dims()
    dims.local_scen, dims.periods = local_scen, periods
    dims.scen_devices, dims.gen_devices = scen_devices, gen_devices
    dims.total_scen = total_scen
    dims.mean_level = float(all_levels.mean())
    dims.level_sq = float((all_levels**2).sum())
    dims.entries = float(total_scen * periods * gens)
    dims.zone_entries = float(total_scen * periods * zones)
    dims.zone_scale = zones / gens

    load = zone_load.reshape(rows, zones)
    diag, cap, zone = (v.reshape(1, local_gen) for v in (cost_diag, capacity, zone_index))
    mask = block_map.reshape(blocks)
    sizes = step_numer.astype(F32) / step_denom.astype(F32)
    sizes = lax.optimization_barrier(jnp.broadcast_to(sizes[:, None, None], (iters, 8, LANES)))

    shape = jax.ShapeDtypeStruct
    dma = pltpu.SemaphoreType.DMA

    per = divisor(blocks, 2)
    width = per * tile
    chunks = blocks // per
    lane_tiles = local_gen // LANES

    cost_c = cost_tiles.reshape(chunks, per, tile, tile)
    coup_c = coupling_tiles.reshape(chunks, per, tile, tile)
    state = shape((chunks, rows, width), F32)
    buffer = pltpu.VMEM((chunks, rows, width), F32)
    part_shape = shape((8, LANES), F32)
    plan_shape = shape((periods, local_gen), F32)
    vector = [linear_cost, diag, cap, zone]
    col_shape = shape((lane_tiles, periods, LANES), F32)
    coef_shape = shape((16 + 8 * iters, LANES), F32)
    grid_shape = shape((rows, zones), F32)

    def exchange(x):
        return lax.all_to_all(x, ("scen", "gen"), 0, 0)

    pack_rows = -(-(1 + 2 * (zones // LANES)) // 8) * 8
    tiles = pltpu.VMEM((chunks, per, tile, tile), BF16)
    base, packed = staged_call(
        functools.partial(first_body, dims), [mask], [], [load] + vector, [cost_c, coup_c],
        [shape((local_scen, local_gen), F32), shape((devices, pack_rows, LANES), F32)], [],
        [
            pltpu.VMEM((8, tile), F32), pltpu.VMEM((24, zones), F32), tiles, tiles,
            dma((2, chunks)),
        ],
        "first", limit=60,
    )
    recv = exchange(packed)

    col_sums, prices, totals, coef, dispatch = staged_call(
        functools.partial(start_body, dims), [], [recv], [sizes, far_away(load), far_away(base)] + vector, [],
        [col_shape, grid_shape, grid_shape, coef_shape], [state], [buffer, dma((chunks,))],
        "start",
    )

    past = [dispatch]
    nothing = lax.optimization_barrier(jnp.zeros((8, LANES), F32))
    odd = lax.axis_index("gen") % 2
    pieces = col_shape.shape[0] * periods // 8
    padded = -(-pieces // scen_devices) * scen_devices
    half_rows = rows // 2
    my_load = lax.dynamic_slice_in_dim(load, odd * half_rows, half_rows, 0)
    swap = [(i, i ^ 1) for i in range(gen_devices)]
    first_half = chunks // 2
    parts = [(0, first_half), (first_half, chunks - first_half)] if first_half else [(0, chunks)]

    for k in range(1, iters):
        last = k == iters - 1
        flat = col_sums.reshape(pieces, 8, LANES)
        if padded != pieces:
            flat = jnp.pad(flat, ((0, padded - pieces), (0, 0), (0, 0)))
        flat = flat.reshape(scen_devices, padded // scen_devices, 8, LANES)
        got = lax.all_to_all(flat, "scen", 0, 0)
        other = lax.ppermute(totals, "gen", swap)

        cols = []
        resid = weight = None
        partial = nothing
        for part, (begin, count) in enumerate(parts):
            part_buffer = pltpu.VMEM((count, rows, width), F32)
            weights = pltpu.VMEM((count, per, tile, tile), BF16)
            carry = [resid, weight] if part else []
            col_k, partial, resid, weight = staged_call(
                functools.partial(hidden_body, dims, k, last, begin, count),
                [mask], [], [coef, prices, partial] + vector, [*past, cost_c, coup_c, *carry],
                [shape((count * width // LANES, periods, LANES), F32), part_shape], [state, state],
                [
                    pltpu.VMEM((rows, zones), BF16), pltpu.VMEM((rows, zones), BF16),
                    pltpu.VMEM((2, periods, LANES), F32),
                ] + [part_buffer] * (k + 2) + [weights, weights, dma((k + 2, count)), dma((2, count))],
                "hidden",
                estimate(count * 24 * rows * tile * tile, count * 8 * rows * width * 4),
                {k + 2 + j: j for j in range(len(carry))},
            )
            cols.append(col_k)
            if part == 0:
                got, partial = lax.optimization_barrier((got, partial))
                piece = pl.pallas_call(
                    piece_kernel, out_shape=shape(got.shape, F32), compiler_params=params(4), name="piece"
                )(got)
                piece, partial = lax.optimization_barrier((piece, partial))
                gathered = lax.all_to_all(piece, "scen", 0, 0)

                totals = totals + other
                near = lax.dynamic_slice_in_dim(totals, odd * half_rows, half_rows, 0)
                far = jnp.zeros_like(near)
                bit = 2
                while bit < gen_devices:
                    if bit > 2:
                        near = near + far
                    far = lax.ppermute(near, "gen", [(i, i ^ bit) for i in range(gen_devices)])
                    bit *= 2

        far, partial = lax.optimization_barrier((far, partial))
        plan = gathered.reshape(padded, 8, LANES)[:pieces].reshape(lane_tiles, periods, LANES)
        mine, primal = pl.pallas_call(
            functools.partial(imbalance_kernel, dims.zone_scale, 2.0 / gen_devices),
            out_shape=[shape((half_rows, zones), F32), shape((8, LANES), F32)],
            compiler_params=params(4),
            name="imbalance",
        )(near, far, my_load)
        other = lax.ppermute(mine, "gen", swap)
        imbalance = jnp.where(
            odd == 0, jnp.concatenate([mine, other]), jnp.concatenate([other, mine])
        )

        (packed,) = staged_call(
            functools.partial(pack_body, dims), [], [plan, primal], [far_away(v) for v in (partial, *cols)], [],
            [shape((devices, 1, LANES), F32)], [], [], "pack", limit=4,
        )
        recv = exchange(packed)

        near, small = [recv], [imbalance, sizes, coef, prices, plan, cap, zone]
        large = [dispatch, resid, weight]
        scratch = [buffer] * 3 + [pltpu.VMEM((8, LANES), F32), dma((3, chunks)), dma((chunks,))]
        cost = estimate(rows * local_gen * 8, rows * local_gen * 16)
        body = functools.partial(update_body, dims, k, last)
        if last:
            prices, plan, dispatch = staged_call(
                body, [], near, small, large, [grid_shape, plan_shape], [shape((rows, local_gen), F32)],
                scratch, "update", cost,
            )
        else:
            prices, col_sums, totals, coef, dispatch = staged_call(
                body, [], near, small, large, [grid_shape, col_shape, grid_shape, coef_shape], [state],
                scratch, "update", cost,
            )
            past.append(dispatch)

    return (
        dispatch.reshape(local_scen, periods, local_gen),
        prices.reshape(local_scen, periods, zones),
        plan,
    )


def solution(mesh):
    placed = (
        P("scen", None, None),
        P(None, "gen"),
        P("gen"),
        P("gen"),
        P("gen", None, None),
        P("scen", "gen", None, None),
        P("scen", "gen"),
        P("gen"),
        P(),
        P(),
    )
    return jax.shard_map(
        local,
        mesh=mesh,
        in_specs=placed,
        out_specs=(P("scen", None, "gen"), P("scen", None, None), P(None, "gen")),
        check_vma=False,
    )
```
